32 devices in a mesh: seq: 8 (over y, x, core), head: 4 (over z).
Axes of the slice: x: 2, y: 2, z: 4, core: 2. Of those that a mesh axis runs over, the one named last changes fastest.
Arguments:
- queries: bfloat16 [2048, 1024], P('seq', 'head'), may hold values from -6 to 6
- keys: bfloat16 [2048, 1024], P('seq', 'head'), may hold values from -6 to 6
- values: bfloat16 [2048, 1024], P('seq', 'head'), may hold values from -6 to 6
- gate: bfloat16 [2048, 1024], P('seq', 'head'), may hold values from -6 to 6
- log_forget: float32 [8, 2048], P('head', 'seq'), may hold values from -1.5 to 0
- write_rate: float32 [8, 2048], P('head', 'seq'), may hold values from 0 to 1
- level_weight: float32 [8, 6, 2048], P('head', None, 'seq'), may hold values from 0.25 to 2.5
- w_out: bfloat16 [1024, 4096], P('head'), may hold values from -0.1875 to 0.1875
Outputs:
- mixed: bfloat16 [2048, 4096], P(('seq', 'head'))
The draws below stay inside these ranges and needn't reach their ends.
All inputs are finite; a program needn't handle non-finite values.
Results may differ from the reference program's by a relative error of at most 0.02.
Values may be sent and summed in bfloat16 or wider, within the bound.
A program may use at most 64 MiB of HBM per device.

```python
import math
import jax
import jax.numpy as jnp
from jax import lax

D = 4096
DK = 128
HEAD_DEV = 2
BLOCK = 64
TOK_DEV = 256
HEADS = 8
TOKENS = 2048
LEVELS = 6
N_HEAD = 4


def draw_log_forget(key, part):
    streams = jax.random.split(key, 5)
    slowest = 0.1 / TOKENS
    fastest = 1.0 / 40.0
    spread = jax.random.uniform(streams[0], (HEADS, 1), jnp.float32)
    update_speeds = jnp.exp(jnp.log(slowest) + spread * (jnp.log(fastest) - jnp.log(slowest)))
    slabs = TOKENS // TOK_DEV
    section_factor = jnp.exp(jax.random.uniform(streams[1], (HEADS, slabs), jnp.float32, -0.6931, 0.6931))
    section_factor = jnp.repeat(section_factor, TOK_DEV, axis=1)
    approximate_guess = jax.random.uniform(streams[2], (HEADS, TOKENS), jnp.float32, 0.5, 1.5)
    chosen_locations = jax.random.randint(streams[3], (2,), 0, TOKENS)
    fading_falls = jax.random.uniform(streams[4], (2,), jnp.float32, -0.6931, -0.2231)
    item_indices = jnp.arange(TOKENS)
    sudden_jumps = jnp.where(item_indices == chosen_locations[0], fading_falls[0], 0.0) + jnp.where(item_indices == chosen_locations[1], fading_falls[1], 0.0)
    return -(update_speeds * section_factor * approximate_guess) + sudden_jumps[None, :]


def draw_write_rate(key, part):
    streams = jax.random.split(jax.random.fold_in(key, 17), 3)
    centers = jax.random.uniform(streams[0], (HEADS, 1), jnp.float32, -6.0, 1.0)
    noise = 0.75 * jax.random.normal(streams[2], (HEADS, TOKENS), jnp.float32)
    return jax.nn.sigmoid(centers + noise).astype(jnp.float32)


def block_scale(own_key, shape, shards, smallest, high):
    factor_of = 1.0
    for position, blocks in shards:
        heights = jax.random.uniform(jax.random.fold_in(jax.random.fold_in(own_key, 6), position), (blocks,), jnp.float32, smallest / len(shards), high / len(shards))
        factor_of = factor_of * jnp.repeat(jnp.exp(heights), shape[position] // blocks).reshape((-1,) + (1,) * (len(shape) - 1 - position))
    return factor_of


def scatter_about(key, extent, scale, reach, cuts=(), kind=jnp.bfloat16):
    values = jax.random.normal(key, extent, jnp.float32) * scale
    if len(cuts) > 0:
        values = block_scale(key, extent, cuts, -0.22, 0.18) * values
    return jnp.clip(values, min=-reach, max=reach).astype(kind)


def setup_inputs(seed: int = 0) -> dict:
    streams_of = jax.random.split(jax.random.key(seed), 9)
    return {
        "queries": scatter_about(streams_of[0], (TOKENS, HEADS * DK), 1.0, 6.0, ((0, 8), (1, 4))),
        "keys": scatter_about(streams_of[1], (TOKENS, HEADS * DK), 1.0, 6.0, ((0, 8), (1, 4))),
        "values": scatter_about(streams_of[2], (TOKENS, HEADS * DK), 1.0, 6.0, ((0, 8), (1, 4))),
        "gate": scatter_about(streams_of[3], (TOKENS, HEADS * DK), 1.0, 6.0, ((0, 8), (1, 4))),
        "log_forget": draw_log_forget(jax.random.fold_in(streams_of[8], 71), 0),
        "write_rate": draw_write_rate(jax.random.fold_in(streams_of[8], 71), 0),
        "level_weight": jnp.clip(jnp.exp(math.log(2.5) - 2.3025851 * jax.random.uniform(streams_of[6], (HEADS, LEVELS, TOKENS), jnp.float32) ** block_scale(streams_of[6], (HEADS, LEVELS, TOKENS), ((0, 4), (2, 8)), -0.2, 0.2)), 0.25, 2.5),
        "w_out": scatter_about(streams_of[7], (HEADS * DK, D), (HEADS * DK) ** -0.5, 0.1875, ((0, 4),)),
    }


EPSILON = 1e-06
PRECISE = lax.Precision.HIGHEST

def unit_rows(matrix):
    floated = matrix.astype(jnp.float32)
    return floated * lax.rsqrt(lax.optimization_barrier(jnp.sum(floated * floated, axis=-1, keepdims=True)) + EPSILON)

def token_step(carried, inputs):
    memory, product = carried
    query_row, key_row, value_row, retain, strength = inputs
    prod_key = jnp.einsum('hij,hj->hi', product, key_row, precision=PRECISE)
    product = retain[:, None, None] * (product - strength[:, None, None] * prod_key[:, :, None] * key_row[:, None, :])
    mem_key = jnp.einsum('hij,hj->hi', memory, key_row, precision=PRECISE)
    memory = retain[:, None, None] * (memory - strength[:, None, None] * mem_key[:, :, None] * key_row[:, None, :])
    memory = memory + strength[:, None, None] * value_row[:, :, None] * key_row[:, None, :]
    reach_row = jnp.einsum('hij,hj->hi', product, query_row, precision=PRECISE)
    own_row = jnp.einsum('hij,hj->hi', memory, query_row, precision=PRECISE)
    return ((memory, product), (reach_row, own_row))

def reference(queries, keys, values, gate, log_forget, write_rate, level_weight, w_out):
    groups = TOKENS // BLOCK
    level_count = LEVELS - 1
    query_rows = unit_rows(queries.reshape(TOKENS, HEADS, DK)).reshape(groups, BLOCK, HEADS, DK)
    key_rows = unit_rows(keys.reshape(TOKENS, HEADS, DK)).reshape(groups, BLOCK, HEADS, DK)
    value_rows = values.astype(jnp.float32).reshape(groups, BLOCK, HEADS, DK)
    retain = jnp.exp(log_forget).T.reshape(groups, BLOCK, HEADS)
    strength = write_rate.T.reshape(groups, BLOCK, HEADS)
    weights = jnp.transpose(level_weight, (2, 0, 1)).reshape(groups, BLOCK, HEADS, LEVELS)
    level_axis = jnp.arange(level_count, dtype=jnp.int32)
    identity = jnp.broadcast_to(jnp.eye(DK, dtype=jnp.float32), (HEADS, DK, DK))

    def block_step(stored, inputs):
        block_queries, block_keys, block_values, block_retain, block_strength, block_weights, ordinal = inputs
        start = (jnp.zeros((HEADS, DK, DK), jnp.float32), identity)
        (ending, moving), (reach_rows, own_rows) = lax.scan(token_step, start, (block_queries, block_keys, block_values, block_retain, block_strength))
        level_reads = jnp.einsum('hlvk,chk->chlv', stored, reach_rows, precision=PRECISE)
        core_rows = block_weights[:, :, 0, None] * own_rows
        core_rows = core_rows + jnp.einsum('chl,chlv->chv', block_weights[:, :, 1:], level_reads, precision=PRECISE)
        merge_level = jnp.int32(0)
        for exponent in range(1, level_count + 1):
            merge_level = merge_level + ((ordinal + 1) % 2 ** exponent == 0).astype(jnp.int32)
        below_mask = (level_axis < merge_level)[None, :, None, None]
        equal_mask = (level_axis == merge_level)[None, :, None, None]
        above_mask = (level_axis > merge_level)[None, :, None, None]
        merged = lax.optimization_barrier(jnp.sum(jnp.where(below_mask, stored, 0.0), axis=1, keepdims=True))
        carried = jnp.where(above_mask, stored, jnp.where(equal_mask, merged, 0.0))
        carried = jnp.einsum('hlij,hjk->hlik', carried, moving, precision=PRECISE)
        carried = carried + jnp.where(equal_mask, ending[:, None], 0.0)
        return (carried, core_rows)
    initial = jnp.zeros((HEADS, level_count, DK, DK), jnp.float32)
    ordinals = jnp.arange(groups, dtype=jnp.int32)
    _, cores = lax.scan(block_step, initial, (query_rows, key_rows, value_rows, retain, strength, weights, ordinals))
    cores = cores.reshape(TOKENS, HEADS, DK)
    scaled = cores * lax.rsqrt(lax.optimization_barrier(jnp.mean(cores * cores, axis=-1, keepdims=True)) + EPSILON)
    gated = scaled * jax.nn.silu(gate.astype(jnp.float32).reshape(TOKENS, HEADS, DK))
    normed = gated.reshape(TOKENS, HEADS * DK).astype(jnp.bfloat16)
    group_width = HEAD_DEV * DK
    pieces = jnp.transpose(normed.reshape(TOKENS, N_HEAD, group_width), (1, 0, 2))
    group_weights = w_out.reshape(N_HEAD, group_width, D)

    def add_group(running, inputs):
        group_rows, group_matrix = inputs
        partial_value = jnp.dot(group_rows, group_matrix, preferred_element_type=jnp.float32).astype(jnp.bfloat16)
        return (running + partial_value.astype(jnp.float32), None)
    running, _ = lax.scan(add_group, jnp.zeros((TOKENS, D), jnp.float32), (pieces, group_weights))
    return running.astype(jnp.bfloat16)
```

```python
import functools

import jax
import jax.numpy as jnp
from jax import lax
from jax.experimental import pallas as pl
from jax.experimental.pallas import tpu as pltpu
from jax.sharding import PartitionSpec as P

DK = 128
BLOCK = 64
EPSILON = 1e-06
F32 = jnp.float32
BF16 = jnp.bfloat16
MESH = pl.DeviceIdType.MESH


def dot(left, right):
    return jnp.dot(left.astype(BF16), right.astype(BF16), preferred_element_type=F32)


def dot_nt(left, right):
    return lax.dot_general(
        left.astype(BF16), right.astype(BF16), (((1,), (1,)), ((), ())), preferred_element_type=F32
    )


def unit_rows(ref, cols):
    floated = ref[:, cols].astype(F32)
    return floated * lax.rsqrt(jnp.sum(floated * floated, axis=-1, keepdims=True) + EPSILON)


def kernel(
    ns, nz, heads, levels,
    q_ref, k_ref, v_ref, g_ref, lf_ref, wr_ref, lw_ref, w_ref, o_ref,
    stage, wbuf, ebuf, pbuf, tbuf, sbuf, hbuf, pm, mbuf, nbuf, gbuf, ybuf, obuf,
    wl_sem, ws_sem, wr_sem, ds_sem, dr_sem, ps_sem, pr_sem, ss_sem, sr_sem,
    ns_sem, nr_sem, gs_sem, gr_sem, os_sem, or_sem,
):
    tok = q_ref.shape[0]
    nq = ns // 2
    width = wbuf.shape[2]
    half = width // 2
    rows = tok // nz
    inner_bits = (tok // BLOCK).bit_length() - 1
    chip_bits = nq.bit_length() - 1
    s = lax.axis_index("seq")
    z = lax.axis_index("head")
    q = s // 2
    c = lax.rem(s, 2)
    partner = s + 1 - 2 * c

    def to(seq, head):
        return {"device_id": (seq, head), "device_id_type": MESH}

    def zpeer(d):
        return lax.rem(z + d, nz)

    def zfrom(d):
        return lax.rem(z + nz - d, nz)

    def qpeer(d):
        return 2 * lax.rem(q + d, nq) + c

    def qfrom(d):
        return lax.rem(q + nq - d, nq)

    barrier = pltpu.get_barrier_semaphore()
    for d in range(1, nz):
        pl.semaphore_signal(barrier, inc=1, **to(s, zpeer(d)))
    pl.semaphore_signal(barrier, inc=1, **to(partner, z))
    for d in range(1, nq):
        pl.semaphore_signal(barrier, inc=1, **to(qpeer(d), z))

    chip_cols = pl.ds(pl.multiple_of(q * width, width), width)
    mine = pl.ds(pl.multiple_of(s * half, half), half)
    my_half = pl.ds(pl.multiple_of(c * half, half), half)
    local_w = pltpu.make_async_copy(w_ref.at[:, chip_cols], wbuf.at[z], wl_sem)
    local_w.start()
    pl.semaphore_wait(barrier, nz + nq - 1)

    w_copies = [
        pltpu.make_async_remote_copy(
            w_ref.at[:, mine], wbuf.at[z, :, my_half], ws_sem.at[d - 1], wr_sem.at[d - 1],
            **to(s, zpeer(d)),
        )
        for d in range(1, nz)
    ]
    for copy in w_copies:
        copy.start()

    stage[...] = jnp.zeros_like(stage)
    stage[0:heads, :] = lf_ref[...]
    ti = lax.broadcasted_iota(jnp.int32, (tok, tok), 0)
    ui = lax.broadcasted_iota(jnp.int32, (tok, tok), 1)
    upto = jnp.where(ti <= ui, 1.0, 0.0).astype(F32)
    stage[0:8, :] = jnp.dot(
        stage[0:8, :], upto, precision=lax.Precision.HIGHEST, preferred_element_type=F32
    )
    stage[8 : 8 + heads, :] = wr_ref[...]
    for h in range(heads):
        stage[16 + h * levels : 16 + (h + 1) * levels, :] = lw_ref[h]
    cols = stage[...].T
    differ = lax.bitwise_xor(ti, ui)
    inclusive = ti >= ui

    hs = range(heads)
    span = [slice(h * DK, (h + 1) * DK) for h in hs]
    c_col = [cols[:, h : h + 1] for h in hs]
    b_col = [cols[:, 8 + h : 9 + h] for h in hs]

    def weight(h, level):
        at = 16 + h * levels + level
        return cols[:, at : at + 1]

    kn = [unit_rows(k_ref, span[h]) for h in hs]
    qn = [unit_rows(q_ref, span[h]) for h in hs]
    kb = [kn[h].astype(BF16) for h in hs]
    low = [jnp.where(ti > ui, b_col[h] * dot_nt(kb[h], kb[h]), 0.0) for h in hs]
    eye = jnp.where(ti == ui, 1.0, 0.0).astype(F32)
    inv = [eye - jnp.where(differ == 1, low[h], 0.0) for h in hs]
    bit = 1
    while 2**bit < tok:
        part = [jnp.where(differ >> bit == 1, low[h], 0.0) for h in hs]
        step = [dot(part[h], inv[h]) for h in hs]
        inv = [inv[h] - dot(inv[h], step[h]) for h in hs]
        bit += 1
    for h in hs:
        low_hi = low[h].astype(BF16)
        low_lo = (low[h] - low_hi.astype(F32)).astype(BF16)
        inv_hi = inv[h].astype(BF16)
        inv_lo = (inv[h] - inv_hi.astype(F32)).astype(BF16)
        residual = eye - inv[h] - (dot(low_hi, inv_hi) + (dot(low_hi, inv_lo) + dot(low_lo, inv_hi)))
        inv[h] = inv[h] + dot(inv_hi, residual)
    fade = [
        jnp.exp(jnp.where(inclusive, c_col[h] - stage[h : h + 1, :], -1e30)) for h in hs
    ]
    bk = [b_col[h] * kn[h] for h in hs]
    bv = [b_col[h] * v_ref[:, span[h]].astype(F32) for h in hs]
    eye_k = jnp.where(
        lax.broadcasted_iota(jnp.int32, (DK, DK), 0) == lax.broadcasted_iota(jnp.int32, (DK, DK), 1),
        1.0, 0.0,
    ).astype(F32)
    for h in hs:
        last = stage[h : h + 1, tok - 1 : tok]
        bases = dot(inv[h], bk[h])
        writes = dot(inv[h] * fade[h], bv[h])
        tail = jnp.exp(last - c_col[h])
        ebuf[h, 0] = dot((writes * tail).T, kb[h]).astype(BF16)
        ebuf[h, 1] = (jnp.exp(last) * (eye_k - dot(bases.T, kb[h]))).astype(BF16)
    pair = pltpu.make_async_remote_copy(ebuf, pbuf, ps_sem, pr_sem, **to(partner, z))
    pair.start()
    reads = [dot(jnp.where(inclusive, dot_nt(qn[h], kb[h]), 0.0), inv[h]) for h in hs]
    lifted = [jnp.exp(c_col[h]) * (qn[h] - dot(reads[h], bk[h])) for h in hs]
    core = []
    for h in hs:
        spread = weight(h, inner_bits)
        for level in reversed(range(inner_bits)):
            spread = jnp.where(differ < BLOCK * 2**level, weight(h, level), spread)
        core.append(dot(reads[h] * fade[h] * spread, bv[h]))

    pair.wait_recv()
    odd = c == 1
    for h in hs:
        e_own, m_own = ebuf[h, 0].astype(F32), ebuf[h, 1].astype(F32)
        e_oth, m_oth = pbuf[h, 0].astype(F32), pbuf[h, 1].astype(F32)
        e_a, e_b = jnp.where(odd, e_oth, e_own), jnp.where(odd, e_own, e_oth)
        m_a, m_b = jnp.where(odd, m_oth, m_own), jnp.where(odd, m_own, m_oth)
        tbuf[h, 0] = (dot(e_a, m_b) + e_b).astype(BF16)
        tbuf[h, 1] = dot(m_a, m_b).astype(BF16)
        hbuf[h, 0] = jnp.where(odd, e_oth, 0.0)
        for level in range(1, chip_bits + 1):
            hbuf[h, level] = jnp.zeros((DK, DK), F32)
        pm[h] = jnp.where(odd, m_oth, eye_k)

    def state_copy(d):
        return pltpu.make_async_remote_copy(
            tbuf, sbuf.at[d - 1], ss_sem.at[d - 1], sr_sem.at[d - 1], **to(qpeer(d), z)
        )

    for d in range(1, nq):
        @pl.when(q + d < nq)
        def _():
            state_copy(d).start()

    gates = []
    for h in hs:
        u = g_ref[:, span[h]].astype(F32)
        gates.append(u / (1.0 + jnp.exp(-u)))

    for d in range(1, nq):
        @pl.when(q >= d)
        def _():
            state_copy(d).wait_recv()
            source = q - d
            level = 0
            for k in range(chip_bits):
                level = level + (source // 2**k != q // 2**k).astype(jnp.int32)
            for h in hs:
                chain = pm[h].astype(BF16)
                hbuf[h, level] += dot(sbuf[d - 1, h, 0], chain)
                pm[h] = dot(sbuf[d - 1, h, 1], chain)

    for h in hs:
        total = core[h]
        for level in range(chip_bits + 1):
            total = total + weight(h, inner_bits + 1 + level) * dot_nt(lifted[h], hbuf[h, level])
        scaled = total * lax.rsqrt(jnp.mean(total * total, axis=-1, keepdims=True) + EPSILON)
        gated = (scaled * gates[h]).astype(BF16)
        for part in range(nz):
            mbuf[part, :, span[h]] = gated[part * rows : (part + 1) * rows]

    n_copies = [
        pltpu.make_async_remote_copy(
            mbuf.at[zpeer(d)], nbuf.at[z], ns_sem.at[d - 1], nr_sem.at[d - 1], **to(s, zpeer(d))
        )
        for d in range(1, nz)
    ]
    for copy in n_copies:
        copy.start()
    nbuf[z] = mbuf[z]

    def w_pass(d):
        place = wbuf.at[zfrom(d), :, my_half]
        return pltpu.make_async_remote_copy(
            place, place, ds_sem.at[d - 1], dr_sem.at[d - 1], **to(partner, z)
        )

    local_w.wait()
    for d in range(1, nz):
        w_copies[d - 1].wait_recv()
        w_pass(d).start()
    for d in range(1, nz):
        n_copies[d - 1].wait_recv()

    g_copies = [
        pltpu.make_async_remote_copy(
            nbuf, gbuf.at[d - 1], gs_sem.at[d - 1], gr_sem.at[d - 1], **to(qpeer(d), z)
        )
        for d in range(1, nq)
    ]
    for copy in g_copies:
        copy.start()
    for d in range(1, nz):
        w_pass(d).wait_recv()

    def project(source):
        total = None
        for group in range(nz):
            share = jnp.dot(source[group], wbuf[group], preferred_element_type=F32)
            share = share.astype(BF16).astype(F32)
            total = share if total is None else total + share
        return total.astype(BF16)

    out_copies = []
    for d in range(1, nq):
        g_copies[d - 1].wait_recv()
        ybuf[d - 1] = project(gbuf.at[d - 1])
        copy = pltpu.make_async_remote_copy(
            ybuf.at[d - 1], obuf.at[q], os_sem.at[d - 1], or_sem.at[nq - d - 1],
            **to(2 * qfrom(d) + c, z),
        )
        copy.start()
        out_copies.append(copy)
    obuf[q] = project(nbuf)
    for d in range(1, nq):
        pltpu.make_async_remote_copy(
            ybuf.at[d - 1], obuf.at[qfrom(d)], os_sem.at[d - 1], or_sem.at[d - 1], **to(qpeer(d), z)
        ).wait_recv()
    for chip in range(nq):
        o_ref[:, chip * width : (chip + 1) * width] = obuf[chip]

    for copy in w_copies + n_copies + g_copies + out_copies + [pair]:
        copy.wait_send()
    for d in range(1, nz):
        w_pass(d).wait_send()
    for d in range(1, nq):
        @pl.when(q + d < nq)
        def _():
            state_copy(d).wait_send()


def solution(mesh):
    ns, nz = mesh.shape["seq"], mesh.shape["head"]
    nq = ns // 2
    chip_bits = nq.bit_length() - 1

    def on_device(queries, keys, values, gate, log_forget, write_rate, level_weight, w_out):
        tok, feats = queries.shape
        heads = log_forget.shape[0]
        levels = level_weight.shape[1]
        model = w_out.shape[1]
        width = model // nq
        rows = tok // nz
        state = (heads, 2, DK, DK)
        dma = pltpu.SemaphoreType.DMA
        vmem = pl.BlockSpec(memory_space=pltpu.VMEM)
        return pl.pallas_call(
            functools.partial(kernel, ns, nz, heads, levels),
            out_shape=jax.ShapeDtypeStruct((rows, model), BF16),
            in_specs=[vmem] * 7 + [pl.BlockSpec(memory_space=pl.ANY)],
            out_specs=vmem,
            scratch_shapes=[
                pltpu.VMEM((128, tok), F32),
                pltpu.VMEM((nz, w_out.shape[0], width), BF16),
                pltpu.VMEM(state, BF16),
                pltpu.VMEM(state, BF16),
                pltpu.VMEM(state, BF16),
                pltpu.VMEM((nq - 1,) + state, BF16),
                pltpu.VMEM((heads, chip_bits + 1, DK, DK), F32),
                pltpu.VMEM((heads, DK, DK), F32),
                pltpu.VMEM((nz, rows, feats), BF16),
                pltpu.VMEM((nz, rows, feats), BF16),
                pltpu.VMEM((nq - 1, nz, rows, feats), BF16),
                pltpu.VMEM((nq - 1, rows, width), BF16),
                pltpu.VMEM((nq, rows, width), BF16),
                dma,
                dma((nz - 1,)),
                dma((nz - 1,)),
                dma((nz - 1,)),
                dma((nz - 1,)),
                dma,
                dma,
                dma((nq - 1,)),
                dma((nq - 1,)),
                dma((nz - 1,)),
                dma((nz - 1,)),
                dma((nq - 1,)),
                dma((nq - 1,)),
                dma((nq - 1,)),
                dma((nq - 1,)),
            ],
            compiler_params=pltpu.CompilerParams(collective_id=0, has_side_effects=True),
            name="fenwick_layer",
        )(queries, keys, values, gate, log_forget, write_rate, level_weight, w_out)

    in_specs = (
        P("seq", "head"),
        P("seq", "head"),
        P("seq", "head"),
        P("seq", "head"),
        P("head", "seq"),
        P("head", "seq"),
        P("head", None, "seq"),
        P("head", None),
    )
    out_specs = P(("seq", "head"), None)
    return jax.shard_map(
        on_device, mesh=mesh, in_specs=in_specs, out_specs=out_specs, check_vma=False
    )
```

```python
import functools

import jax
import jax.numpy as jnp
from jax import lax
from jax.experimental import pallas as pl
from jax.experimental.pallas import tpu as pltpu
from jax.sharding import PartitionSpec as P

DK = 128
BLOCK = 64
EPSILON = 1e-06
F32 = jnp.float32
BF16 = jnp.bfloat16
MESH = pl.DeviceIdType.MESH


def dot(left, right):
    return jnp.dot(left.astype(BF16), right.astype(BF16), preferred_element_type=F32)


def dot_nt(left, right):
    return lax.dot_general(
        left.astype(BF16), right.astype(BF16), (((1,), (1,)), ((), ())), preferred_element_type=F32
    )


def unit_rows(ref, cols):
    floated = ref[:, cols].astype(F32)
    return floated * lax.rsqrt(jnp.sum(floated * floated, axis=-1, keepdims=True) + EPSILON)


def kernel(
    ns, nz, heads, levels,
    q_ref, k_ref, v_ref, g_ref, lf_ref, wr_ref, lw_ref, w_ref, o_ref,
    stage, wbuf, wrest, xbuf, rbuf, ebuf, pbuf, tbuf, sbuf, hbuf, pm, mbuf, nbuf, gbuf, ybuf, obuf,
    wl_sem, wt_sem, xs_sem, xr_sem, ws_sem, wr_sem, ds_sem, dr_sem, ps_sem, pr_sem, ss_sem, sr_sem,
    ns_sem, nr_sem, gs_sem, gr_sem, os_sem, or_sem,
):
    tok = q_ref.shape[0]
    nq = ns // 2
    width = wbuf.shape[2]
    half = width // 2
    rows = tok // nz
    inner_bits = (tok // BLOCK).bit_length() - 1
    chip_bits = nq.bit_length() - 1
    s = lax.axis_index("seq")
    z = lax.axis_index("head")
    q = s // 2
    c = lax.rem(s, 2)
    partner = s + 1 - 2 * c

    def to(seq, head):
        return {"device_id": (seq, head), "device_id_type": MESH}

    def zpeer(d):
        return lax.rem(z + d, nz)

    def zfrom(d):
        return lax.rem(z + nz - d, nz)

    def qpeer(d):
        return 2 * lax.rem(q + d, nq) + c

    def qfrom(d):
        return lax.rem(q + nq - d, nq)

    barrier = pltpu.get_barrier_semaphore()
    for d in range(1, nz):
        pl.semaphore_signal(barrier, inc=1, **to(s, zpeer(d)))
    pl.semaphore_signal(barrier, inc=1, **to(partner, z))
    for d in range(1, nq):
        pl.semaphore_signal(barrier, inc=1, **to(qpeer(d), z))

    chip_cols = pl.ds(pl.multiple_of(q * width, width), width)
    mine = pl.ds(pl.multiple_of(s * half, half), half)
    my_half = pl.ds(pl.multiple_of(c * half, half), half)
    local_w = pltpu.make_async_copy(w_ref.at[:, chip_cols], wbuf.at[z], wl_sem)
    local_w.start()
    rest = w_ref.shape[1] - nq * width
    if rest:
        local_rest = pltpu.make_async_copy(w_ref.at[:, nq * width :], wrest, wt_sem)
        local_rest.start()
    pl.semaphore_wait(barrier, nz + nq - 1)

    w_copies = [
        pltpu.make_async_remote_copy(
            w_ref.at[:, mine], wbuf.at[z, :, my_half], ws_sem.at[d - 1], wr_sem.at[d - 1],
            **to(s, zpeer(d)),
        )
        for d in range(1, nz)
    ]
    for copy in w_copies:
        copy.start()

    stage[...] = jnp.zeros_like(stage)
    stage[0:heads, :] = lf_ref[...]
    ti = lax.broadcasted_iota(jnp.int32, (tok, tok), 0)
    ui = lax.broadcasted_iota(jnp.int32, (tok, tok), 1)
    upto = jnp.where(ti <= ui, 1.0, 0.0).astype(F32)
    stage[0:8, :] = jnp.dot(
        stage[0:8, :], upto, precision=lax.Precision.HIGHEST, preferred_element_type=F32
    )
    stage[8 : 8 + heads, :] = wr_ref[...]
    for h in range(heads):
        stage[16 + h * levels : 16 + (h + 1) * levels, :] = lw_ref[h]
    cols = stage[...].T
    differ = lax.bitwise_xor(ti, ui)
    inclusive = ti >= ui

    hs = range(heads)
    span = [slice(h * DK, (h + 1) * DK) for h in hs]
    c_col = [cols[:, h : h + 1] for h in hs]
    b_col = [cols[:, 8 + h : 9 + h] for h in hs]

    def weight(h, level):
        at = 16 + h * levels + level
        return cols[:, at : at + 1]

    kn = [unit_rows(k_ref, span[h]) for h in hs]
    qn = [unit_rows(q_ref, span[h]) for h in hs]
    kb = [kn[h].astype(BF16) for h in hs]
    low = [jnp.where(ti > ui, b_col[h] * dot_nt(kb[h], kb[h]), 0.0) for h in hs]
    eye = jnp.where(ti == ui, 1.0, 0.0).astype(F32)
    inv = [eye - jnp.where(differ == 1, low[h], 0.0) for h in hs]
    bit = 1
    while 2**bit < tok:
        part = [jnp.where(differ >> bit == 1, low[h], 0.0) for h in hs]
        step = [dot(part[h], inv[h]) for h in hs]
        inv = [inv[h] - dot(inv[h], step[h]) for h in hs]
        bit += 1
    for h in hs:
        low_hi = low[h].astype(BF16)
        low_lo = (low[h] - low_hi.astype(F32)).astype(BF16)
        inv_hi = inv[h].astype(BF16)
        inv_lo = (inv[h] - inv_hi.astype(F32)).astype(BF16)
        residual = eye - inv[h] - (dot(low_hi, inv_hi) + (dot(low_hi, inv_lo) + dot(low_lo, inv_hi)))
        inv[h] = inv[h] + dot(inv_hi, residual)
    fade = [
        jnp.exp(jnp.where(inclusive, c_col[h] - stage[h : h + 1, :], -1e30)) for h in hs
    ]
    bk = [b_col[h] * kn[h] for h in hs]
    bv = [b_col[h] * v_ref[:, span[h]].astype(F32) for h in hs]
    eye_k = jnp.where(
        lax.broadcasted_iota(jnp.int32, (DK, DK), 0) == lax.broadcasted_iota(jnp.int32, (DK, DK), 1),
        1.0, 0.0,
    ).astype(F32)
    for h in hs:
        last = stage[h : h + 1, tok - 1 : tok]
        bases = dot(inv[h], bk[h])
        writes = dot(inv[h] * fade[h], bv[h])
        tail = jnp.exp(last - c_col[h])
        ebuf[h, 0] = dot((writes * tail).T, kb[h]).astype(BF16)
        ebuf[h, 1] = (jnp.exp(last) * (eye_k - dot(bases.T, kb[h]))).astype(BF16)
    pair = pltpu.make_async_remote_copy(ebuf, pbuf, ps_sem, pr_sem, **to(partner, z))
    pair.start()
    reads = [dot(jnp.where(inclusive, dot_nt(qn[h], kb[h]), 0.0), inv[h]) for h in hs]
    lifted = [jnp.exp(c_col[h]) * (qn[h] - dot(reads[h], bk[h])) for h in hs]
    core = []
    for h in hs:
        spread = weight(h, inner_bits)
        for level in reversed(range(inner_bits)):
            spread = jnp.where(differ < BLOCK * 2**level, weight(h, level), spread)
        core.append(dot(reads[h] * fade[h] * spread, bv[h]))

    pair.wait_recv()
    odd = c == 1
    for h in hs:
        e_own, m_own = ebuf[h, 0].astype(F32), ebuf[h, 1].astype(F32)
        e_oth, m_oth = pbuf[h, 0].astype(F32), pbuf[h, 1].astype(F32)
        e_a, e_b = jnp.where(odd, e_oth, e_own), jnp.where(odd, e_own, e_oth)
        m_a, m_b = jnp.where(odd, m_oth, m_own), jnp.where(odd, m_own, m_oth)
        tbuf[h, 0] = (dot(e_a, m_b) + e_b).astype(BF16)
        tbuf[h, 1] = dot(m_a, m_b).astype(BF16)
        hbuf[h, 0] = jnp.where(odd, e_oth, 0.0)
        for level in range(1, chip_bits + 1):
            hbuf[h, level] = jnp.zeros((DK, DK), F32)
        pm[h] = jnp.where(odd, m_oth, eye_k)

    def state_copy(d):
        return pltpu.make_async_remote_copy(
            tbuf, sbuf.at[d - 1], ss_sem.at[d - 1], sr_sem.at[d - 1], **to(qpeer(d), z)
        )

    for d in range(1, nq):
        @pl.when(q + d < nq)
        def _():
            state_copy(d).start()

    gates = []
    for h in hs:
        u = g_ref[:, span[h]].astype(F32)
        gates.append(u / (1.0 + jnp.exp(-u)))

    for d in range(1, nq):
        @pl.when(q >= d)
        def _():
            state_copy(d).wait_recv()
            source = q - d
            level = 0
            for k in range(chip_bits):
                level = level + (source // 2**k != q // 2**k).astype(jnp.int32)
            for h in hs:
                chain = pm[h].astype(BF16)
                hbuf[h, level] += dot(sbuf[d - 1, h, 0], chain)
                pm[h] = dot(sbuf[d - 1, h, 1], chain)

    for h in hs:
        total = core[h]
        for level in range(chip_bits + 1):
            total = total + weight(h, inner_bits + 1 + level) * dot_nt(lifted[h], hbuf[h, level])
        scaled = total * lax.rsqrt(jnp.mean(total * total, axis=-1, keepdims=True) + EPSILON)
        gated = (scaled * gates[h]).astype(BF16)
        for part in range(nz):
            mbuf[part, :, span[h]] = gated[part * rows : (part + 1) * rows]

    n_copies = [
        pltpu.make_async_remote_copy(
            mbuf.at[zpeer(d)], nbuf.at[z], ns_sem.at[d - 1], nr_sem.at[d - 1], **to(s, zpeer(d))
        )
        for d in range(1, nz)
    ]
    for copy in n_copies:
        copy.start()
    nbuf[z] = mbuf[z]

    x_copies = []
    if rest:
        local_rest.wait()
        for d in range(1, nz):
            share = jnp.dot(mbuf[zpeer(d)], wrest[...], preferred_element_type=F32)
            xbuf[d - 1] = share.astype(BF16)
            copy = pltpu.make_async_remote_copy(
                xbuf.at[d - 1], rbuf.at[d - 1], xs_sem.at[d - 1], xr_sem.at[d - 1],
                **to(s, zpeer(d)),
            )
            copy.start()
            x_copies.append(copy)

    def w_pass(d):
        place = wbuf.at[zfrom(d), :, my_half]
        return pltpu.make_async_remote_copy(
            place, place, ds_sem.at[d - 1], dr_sem.at[d - 1], **to(partner, z)
        )

    local_w.wait()
    for d in range(1, nz):
        w_copies[d - 1].wait_recv()
        w_pass(d).start()
    for d in range(1, nz):
        n_copies[d - 1].wait_recv()

    g_copies = [
        pltpu.make_async_remote_copy(
            nbuf, gbuf.at[d - 1], gs_sem.at[d - 1], gr_sem.at[d - 1], **to(qpeer(d), z)
        )
        for d in range(1, nq)
    ]
    for copy in g_copies:
        copy.start()
    for d in range(1, nz):
        w_pass(d).wait_recv()

    def project(source):
        total = None
        for group in range(nz):
            share = jnp.dot(source[group], wbuf[group], preferred_element_type=F32)
            share = share.astype(BF16).astype(F32)
            total = share if total is None else total + share
        return total.astype(BF16)

    obuf[q] = project(nbuf)
    out_copies = []
    for d in range(1, nq):
        g_copies[d - 1].wait_recv()
        ybuf[d - 1] = project(gbuf.at[d - 1])
        copy = pltpu.make_async_remote_copy(
            ybuf.at[d - 1], obuf.at[q], os_sem.at[d - 1], or_sem.at[nq - d - 1],
            **to(2 * qfrom(d) + c, z),
        )
        copy.start()
        out_copies.append(copy)
    if rest:
        total = jnp.dot(mbuf[z], wrest[...], preferred_element_type=F32).astype(BF16).astype(F32)
        for d in range(1, nz):
            x_copies[d - 1].wait_recv()
            total = total + rbuf[d - 1].astype(F32)
        o_ref[:, nq * width :] = total.astype(BF16)
    for d in range(1, nq):
        pltpu.make_async_remote_copy(
            ybuf.at[d - 1], obuf.at[qfrom(d)], os_sem.at[d - 1], or_sem.at[d - 1], **to(qpeer(d), z)
        ).wait_recv()
    for chip in range(nq):
        o_ref[:, chip * width : (chip + 1) * width] = obuf[chip]

    for copy in w_copies + n_copies + x_copies + g_copies + out_copies + [pair]:
        copy.wait_send()
    for d in range(1, nz):
        w_pass(d).wait_send()
    for d in range(1, nq):
        @pl.when(q + d < nq)
        def _():
            state_copy(d).wait_send()


def solution(mesh):
    ns, nz = mesh.shape["seq"], mesh.shape["head"]
    nq = ns // 2
    chip_bits = nq.bit_length() - 1

    def on_device(queries, keys, values, gate, log_forget, write_rate, level_weight, w_out):
        tok, feats = queries.shape
        heads = log_forget.shape[0]
        levels = level_weight.shape[1]
        model = w_out.shape[1]
        tiles = model // (DK * ns)
        width = 2 * DK * (tiles - tiles // 4)
        rest = max(model - nq * width, DK)
        rows = tok // nz
        state = (heads, 2, DK, DK)
        dma = pltpu.SemaphoreType.DMA
        vmem = pl.BlockSpec(memory_space=pltpu.VMEM)
        return pl.pallas_call(
            functools.partial(kernel, ns, nz, heads, levels),
            out_shape=jax.ShapeDtypeStruct((rows, model), BF16),
            in_specs=[vmem] * 7 + [pl.BlockSpec(memory_space=pl.ANY)],
            out_specs=vmem,
            scratch_shapes=[
                pltpu.VMEM((128, tok), F32),
                pltpu.VMEM((nz, w_out.shape[0], width), BF16),
                pltpu.VMEM((w_out.shape[0], rest), BF16),
                pltpu.VMEM((nz - 1, rows, rest), BF16),
                pltpu.VMEM((nz - 1, rows, rest), BF16),
                pltpu.VMEM(state, BF16),
                pltpu.VMEM(state, BF16),
                pltpu.VMEM(state, BF16),
                pltpu.VMEM((nq - 1,) + state, BF16),
                pltpu.VMEM((heads, chip_bits + 1, DK, DK), F32),
                pltpu.VMEM((heads, DK, DK), F32),
                pltpu.VMEM((nz, rows, feats), BF16),
                pltpu.VMEM((nz, rows, feats), BF16),
                pltpu.VMEM((nq - 1, nz, rows, feats), BF16),
                pltpu.VMEM((nq - 1, rows, width), BF16),
                pltpu.VMEM((nq, rows, width), BF16),
                dma,
                dma,
                dma((nz - 1,)),
                dma((nz - 1,)),
                dma((nz - 1,)),
                dma((nz - 1,)),
                dma((nz - 1,)),
                dma((nz - 1,)),
                dma,
                dma,
                dma((nq - 1,)),
                dma((nq - 1,)),
                dma((nz - 1,)),
                dma((nz - 1,)),
                dma((nq - 1,)),
                dma((nq - 1,)),
                dma((nq - 1,)),
                dma((nq - 1,)),
            ],
            compiler_params=pltpu.CompilerParams(collective_id=0, has_side_effects=True),
            name="fenwick_layer",
        )(queries, keys, values, gate, log_forget, write_rate, level_weight, w_out)

    in_specs = (
        P("seq", "head"),
        P("seq", "head"),
        P("seq", "head"),
        P("seq", "head"),
        P("head", "seq"),
        P("head", "seq"),
        P("head", None, "seq"),
        P("head", None),
    )
    out_specs = P(("seq", "head"), None)
    return jax.shard_map(
        on_device, mesh=mesh, in_specs=in_specs, out_specs=out_specs, check_vma=False
    )
```

```python
import functools

import jax
import jax.numpy as jnp
from jax import lax
from jax.experimental import pallas as pl
from jax.experimental.pallas import tpu as pltpu
from jax.sharding import PartitionSpec as P

DK = 128
BLOCK = 64
EPSILON = 1e-06
F32 = jnp.float32
BF16 = jnp.bfloat16
MESH = pl.DeviceIdType.MESH


def dot(left, right):
    return jnp.dot(left.astype(BF16), right.astype(BF16), preferred_element_type=F32)


def dot_nt(left, right):
    return lax.dot_general(
        left.astype(BF16), right.astype(BF16), (((1,), (1,)), ((), ())), preferred_element_type=F32
    )


def unit_rows(ref, cols):
    floated = ref[:, cols].astype(F32)
    return floated * lax.rsqrt(jnp.sum(floated * floated, axis=-1, keepdims=True) + EPSILON)


def kernel(
    ns, nz, heads, levels,
    q_ref, k_ref, v_ref, g_ref, lf_ref, wr_ref, lw_ref, w_ref, o_ref,
    stage, wbuf, wrest, xbuf, rbuf, ebuf, pbuf, tbuf, sbuf, hbuf, pm, mbuf, nbuf, gbuf, ybuf, obuf,
    wl_sem, wt_sem, xs_sem, xr_sem, ws_sem, wr_sem, ds_sem, dr_sem, ps_sem, pr_sem, ss_sem, sr_sem,
    ns_sem, nr_sem, gs_sem, gr_sem, os_sem, or_sem,
):
    tok = q_ref.shape[0]
    nq = ns // 2
    width = wbuf.shape[2]
    half = width // 2
    rows = tok // nz
    inner_bits = (tok // BLOCK).bit_length() - 1
    chip_bits = nq.bit_length() - 1
    s = lax.axis_index("seq")
    z = lax.axis_index("head")
    q = s // 2
    c = lax.rem(s, 2)
    partner = s + 1 - 2 * c

    def to(seq, head):
        return {"device_id": (seq, head), "device_id_type": MESH}

    def zpeer(d):
        return lax.rem(z + d, nz)

    def zfrom(d):
        return lax.rem(z + nz - d, nz)

    def qpeer(d):
        return 2 * lax.rem(q + d, nq) + c

    def qfrom(d):
        return lax.rem(q + nq - d, nq)

    barrier = pltpu.get_barrier_semaphore()
    for d in range(1, nz):
        pl.semaphore_signal(barrier, inc=1, **to(s, zpeer(d)))
    pl.semaphore_signal(barrier, inc=1, **to(partner, z))
    for d in range(1, nq):
        pl.semaphore_signal(barrier, inc=1, **to(qpeer(d), z))

    chip_cols = pl.ds(pl.multiple_of(q * width, width), width)
    mine = pl.ds(pl.multiple_of(s * half, half), half)
    my_half = pl.ds(pl.multiple_of(c * half, half), half)
    local_w = pltpu.make_async_copy(w_ref.at[:, chip_cols], wbuf.at[z], wl_sem)
    local_w.start()
    rest = w_ref.shape[1] - nq * width
    if rest:
        local_rest = pltpu.make_async_copy(w_ref.at[:, nq * width :], wrest, wt_sem)
        local_rest.start()
    pl.semaphore_wait(barrier, nz + nq - 1)

    w_copies = [
        pltpu.make_async_remote_copy(
            w_ref.at[:, mine], wbuf.at[z, :, my_half], ws_sem.at[d - 1], wr_sem.at[d - 1],
            **to(s, zpeer(d)),
        )
        for d in range(1, nz)
    ]
    for copy in w_copies:
        copy.start()

    stage[...] = jnp.zeros_like(stage)
    stage[0:heads, :] = lf_ref[...]
    ti = lax.broadcasted_iota(jnp.int32, (tok, tok), 0)
    ui = lax.broadcasted_iota(jnp.int32, (tok, tok), 1)
    upto = jnp.where(ti <= ui, 1.0, 0.0).astype(F32)
    stage[0:8, :] = jnp.dot(
        stage[0:8, :], upto, precision=lax.Precision.HIGHEST, preferred_element_type=F32
    )
    stage[8 : 8 + heads, :] = wr_ref[...]
    for level in range(levels):
        stage[16 + level * heads : 16 + (level + 1) * heads, :] = lw_ref[level]
    cols = stage[...].T
    differ = lax.bitwise_xor(ti, ui)
    inclusive = ti >= ui

    hs = range(heads)
    span = [slice(h * DK, (h + 1) * DK) for h in hs]
    c_col = [cols[:, h : h + 1] for h in hs]
    b_col = [cols[:, 8 + h : 9 + h] for h in hs]

    def weight(h, level):
        at = 16 + level * heads + h
        return cols[:, at : at + 1]

    kn = [unit_rows(k_ref, span[h]) for h in hs]
    qn = [unit_rows(q_ref, span[h]) for h in hs]
    kb = [kn[h].astype(BF16) for h in hs]
    low = [jnp.where(ti > ui, b_col[h] * dot_nt(kb[h], kb[h]), 0.0) for h in hs]
    eye = jnp.where(ti == ui, 1.0, 0.0).astype(F32)
    inv = [eye - jnp.where(differ == 1, low[h], 0.0) for h in hs]
    bit = 1
    while 2**bit < tok:
        part = [jnp.where(differ >> bit == 1, low[h], 0.0) for h in hs]
        step = [dot(part[h], inv[h]) for h in hs]
        inv = [inv[h] - dot(inv[h], step[h]) for h in hs]
        bit += 1
    for h in hs:
        low_hi = low[h].astype(BF16)
        low_lo = (low[h] - low_hi.astype(F32)).astype(BF16)
        inv_hi = inv[h].astype(BF16)
        inv_lo = (inv[h] - inv_hi.astype(F32)).astype(BF16)
        residual = eye - inv[h] - (dot(low_hi, inv_hi) + (dot(low_hi, inv_lo) + dot(low_lo, inv_hi)))
        inv[h] = inv[h] + dot(inv_hi, residual)
    fade = [
        jnp.exp(jnp.where(inclusive, c_col[h] - stage[h : h + 1, :], -1e30)) for h in hs
    ]
    bk = [b_col[h] * kn[h] for h in hs]
    bv = [b_col[h] * v_ref[:, span[h]].astype(F32) for h in hs]
    eye_k = jnp.where(
        lax.broadcasted_iota(jnp.int32, (DK, DK), 0) == lax.broadcasted_iota(jnp.int32, (DK, DK), 1),
        1.0, 0.0,
    ).astype(F32)
    for h in hs:
        last = stage[h : h + 1, tok - 1 : tok]
        bases = dot(inv[h], bk[h])
        writes = dot(inv[h] * fade[h], bv[h])
        tail = jnp.exp(last - c_col[h])
        ebuf[h, 0] = dot((writes * tail).T, kb[h]).astype(BF16)
        ebuf[h, 1] = (jnp.exp(last) * (eye_k - dot(bases.T, kb[h]))).astype(BF16)
    pair = pltpu.make_async_remote_copy(ebuf, pbuf, ps_sem, pr_sem, **to(partner, z))
    pair.start()
    reads = [dot(jnp.where(inclusive, dot_nt(qn[h], kb[h]), 0.0), inv[h]) for h in hs]
    lifted = [jnp.exp(c_col[h]) * (qn[h] - dot(reads[h], bk[h])) for h in hs]
    core = []
    for h in hs:
        spread = weight(h, inner_bits)
        for level in reversed(range(inner_bits)):
            spread = jnp.where(differ < BLOCK * 2**level, weight(h, level), spread)
        core.append(dot(reads[h] * fade[h] * spread, bv[h]))

    pair.wait_recv()
    odd = c == 1
    for h in hs:
        e_own, m_own = ebuf[h, 0].astype(F32), ebuf[h, 1].astype(F32)
        e_oth, m_oth = pbuf[h, 0].astype(F32), pbuf[h, 1].astype(F32)
        e_a, e_b = jnp.where(odd, e_oth, e_own), jnp.where(odd, e_own, e_oth)
        m_a, m_b = jnp.where(odd, m_oth, m_own), jnp.where(odd, m_own, m_oth)
        tbuf[h, 0] = (dot(e_a, m_b) + e_b).astype(BF16)
        tbuf[h, 1] = dot(m_a, m_b).astype(BF16)
        hbuf[h, 0] = jnp.where(odd, e_oth, 0.0)
        for level in range(1, chip_bits + 1):
            hbuf[h, level] = jnp.zeros((DK, DK), F32)
        pm[h] = jnp.where(odd, m_oth, eye_k)

    def state_copy(d):
        return pltpu.make_async_remote_copy(
            tbuf, sbuf.at[d - 1], ss_sem.at[d - 1], sr_sem.at[d - 1], **to(qpeer(d), z)
        )

    for d in range(1, nq):
        @pl.when(q + d < nq)
        def _():
            state_copy(d).start()

    gates = []
    for h in hs:
        u = g_ref[:, span[h]].astype(F32)
        gates.append(u / (1.0 + jnp.exp(-u)))

    for d in range(1, nq):
        @pl.when(q >= d)
        def _():
            state_copy(d).wait_recv()
            source = q - d
            level = 0
            for k in range(chip_bits):
                level = level + (source // 2**k != q // 2**k).astype(jnp.int32)
            for h in hs:
                chain = pm[h].astype(BF16)
                hbuf[h, level] += dot(sbuf[d - 1, h, 0], chain)
                pm[h] = dot(sbuf[d - 1, h, 1], chain)

    for h in hs:
        total = core[h]
        for level in range(chip_bits + 1):
            total = total + weight(h, inner_bits + 1 + level) * dot_nt(lifted[h], hbuf[h, level])
        scaled = total * lax.rsqrt(jnp.mean(total * total, axis=-1, keepdims=True) + EPSILON)
        gated = (scaled * gates[h]).astype(BF16)
        for part in range(nz):
            mbuf[part, :, span[h]] = gated[part * rows : (part + 1) * rows]

    n_copies = [
        pltpu.make_async_remote_copy(
            mbuf.at[zpeer(d)], nbuf.at[z], ns_sem.at[d - 1], nr_sem.at[d - 1], **to(s, zpeer(d))
        )
        for d in range(1, nz)
    ]
    for copy in n_copies:
        copy.start()

    order = sorted(range(1, nq), key=lambda d: abs(2 * d - nq))

    def plane_copy(d, e):
        group = zfrom(e)
        return pltpu.make_async_remote_copy(
            nbuf.at[group] if e else mbuf.at[z],
            gbuf.at[d - 1, group],
            gs_sem.at[d - 1, e],
            gr_sem.at[d - 1, e],
            **to(qpeer(d), z),
        )

    for d in order:
        plane_copy(d, 0).start()
    nbuf[z] = mbuf[z]

    x_copies = []
    if rest:
        local_rest.wait()
        for d in range(1, nz):
            share = jnp.dot(mbuf[zpeer(d)], wrest[...], preferred_element_type=F32)
            xbuf[d - 1] = share.astype(BF16)
            copy = pltpu.make_async_remote_copy(
                xbuf.at[d - 1], rbuf.at[d - 1], xs_sem.at[d - 1], xr_sem.at[d - 1],
                **to(s, zpeer(d)),
            )
            copy.start()
            x_copies.append(copy)

    def w_pass(d):
        place = wbuf.at[zfrom(d), :, my_half]
        return pltpu.make_async_remote_copy(
            place, place, ds_sem.at[d - 1], dr_sem.at[d - 1], **to(partner, z)
        )

    for e in range(1, nz):
        n_copies[e - 1].wait_recv()
        for d in order:
            plane_copy(d, e).start()
    local_w.wait()
    for d in range(1, nz):
        w_copies[d - 1].wait_recv()
        w_pass(d).start()
    for d in range(1, nz):
        w_pass(d).wait_recv()

    def project(source):
        total = None
        for group in range(nz):
            share = jnp.dot(source[group], wbuf[group], preferred_element_type=F32)
            share = share.astype(BF16).astype(F32)
            total = share if total is None else total + share
        return total.astype(BF16)

    obuf[q] = project(nbuf)
    out_copies = []
    for d in order:
        for e in range(nz):
            plane_copy(d, e).wait_recv()
        ybuf[d - 1] = project(gbuf.at[d - 1])
        copy = pltpu.make_async_remote_copy(
            ybuf.at[d - 1], obuf.at[q], os_sem.at[d - 1], or_sem.at[nq - d - 1],
            **to(2 * qfrom(d) + c, z),
        )
        copy.start()
        out_copies.append(copy)
    if rest:
        total = jnp.dot(mbuf[z], wrest[...], preferred_element_type=F32).astype(BF16).astype(F32)
        for d in range(1, nz):
            x_copies[d - 1].wait_recv()
            total = total + rbuf[d - 1].astype(F32)
        o_ref[:, nq * width :] = total.astype(BF16)
    for d in range(1, nq):
        pltpu.make_async_remote_copy(
            ybuf.at[d - 1], obuf.at[qfrom(d)], os_sem.at[d - 1], or_sem.at[d - 1], **to(qpeer(d), z)
        ).wait_recv()
    for chip in range(nq):
        o_ref[:, chip * width : (chip + 1) * width] = obuf[chip]

    for copy in w_copies + n_copies + x_copies + out_copies + [pair]:
        copy.wait_send()
    for d in range(1, nz):
        w_pass(d).wait_send()
    for d in range(1, nq):
        for e in range(nz):
            plane_copy(d, e).wait_send()
    for d in range(1, nq):
        @pl.when(q + d < nq)
        def _():
            state_copy(d).wait_send()


def solution(mesh):
    ns, nz = mesh.shape["seq"], mesh.shape["head"]
    nq = ns // 2
    chip_bits = nq.bit_length() - 1

    def on_device(queries, keys, values, gate, log_forget, write_rate, level_weight, w_out):
        tok, feats = queries.shape
        heads = log_forget.shape[0]
        levels = level_weight.shape[1]
        model = w_out.shape[1]
        tiles = model // (DK * ns)
        width = 2 * DK * (tiles - tiles // 4)
        rest = max(model - nq * width, DK)
        rows = tok // nz
        state = (heads, 2, DK, DK)
        dma = pltpu.SemaphoreType.DMA
        vmem = pl.BlockSpec(memory_space=pltpu.VMEM)
        return pl.pallas_call(
            functools.partial(kernel, ns, nz, heads, levels),
            out_shape=jax.ShapeDtypeStruct((rows, model), BF16),
            in_specs=[vmem] * 7 + [pl.BlockSpec(memory_space=pl.ANY)],
            out_specs=vmem,
            scratch_shapes=[
                pltpu.VMEM((128, tok), F32),
                pltpu.VMEM((nz, w_out.shape[0], width), BF16),
                pltpu.VMEM((w_out.shape[0], rest), BF16),
                pltpu.VMEM((nz - 1, rows, rest), BF16),
                pltpu.VMEM((nz - 1, rows, rest), BF16),
                pltpu.VMEM(state, BF16),
                pltpu.VMEM(state, BF16),
                pltpu.VMEM(state, BF16),
                pltpu.VMEM((nq - 1,) + state, BF16),
                pltpu.VMEM((heads, chip_bits + 1, DK, DK), F32),
                pltpu.VMEM((heads, DK, DK), F32),
                pltpu.VMEM((nz, rows, feats), BF16),
                pltpu.VMEM((nz, rows, feats), BF16),
                pltpu.VMEM((nq - 1, nz, rows, feats), BF16),
                pltpu.VMEM((nq - 1, rows, width), BF16),
                pltpu.VMEM((nq, rows, width), BF16),
                dma,
                dma,
                dma((nz - 1,)),
                dma((nz - 1,)),
                dma((nz - 1,)),
                dma((nz - 1,)),
                dma((nz - 1,)),
                dma((nz - 1,)),
                dma,
                dma,
                dma((nq - 1,)),
                dma((nq - 1,)),
                dma((nz - 1,)),
                dma((nz - 1,)),
                dma((nq - 1, nz)),
                dma((nq - 1, nz)),
                dma((nq - 1,)),
                dma((nq - 1,)),
            ],
            compiler_params=pltpu.CompilerParams(collective_id=0, has_side_effects=True),
            name="fenwick_layer",
        )(queries, keys, values, gate, log_forget, write_rate, jnp.swapaxes(level_weight, 0, 1), w_out)

    in_specs = (
        P("seq", "head"),
        P("seq", "head"),
        P("seq", "head"),
        P("seq", "head"),
        P("head", "seq"),
        P("head", "seq"),
        P("head", None, "seq"),
        P("head", None),
    )
    out_specs = P(("seq", "head"), None)
    return jax.shard_map(
        on_device, mesh=mesh, in_specs=in_specs, out_specs=out_specs, check_vma=False
    )
```
